32 devices in a mesh: dp: 8 (over y, x, core), mp: 4 (over z).
Axes of the slice: x: 2, y: 2, z: 4, core: 2. Of those that a mesh axis runs over, the one named last changes fastest.
Arguments:
- tokens: bfloat16 [12288, 4096], P('dp'), may hold values from -40 to 40
- norm_gain: bfloat16 [4096], replicated, may hold values from 0.099609375 to 1.8984375
- w_query: bfloat16 [4096, 2048], P(None, 'mp'), may hold values from -1 to 1
- w_key: bfloat16 [4096, 512], P(None, 'mp'), may hold values from -4 to 4
- w_value: bfloat16 [4096, 512], P(None, 'mp'), may hold values from -0.09375 to 0.09375
- w_out: bfloat16 [2048, 4096], P('mp'), may hold values from -0.125 to 0.125
- seq_starts: int32 [64], P('dp'), may hold values from 0 to 1408, as said below
- seq_lengths: int32 [64], P('dp'), may hold values from 128 to 640
- episode_ids: int32 [64], replicated, may hold values from 0 to 0, as said below
- class_ids: int32 [64], replicated, may hold values from 0 to 31
- query_flags: int32 [64], replicated, may hold values from 0 to 1
Outputs:
- log_probs: float32 [64, 32], P('dp')
- prototypes: float32 [32, 4096], P(None, 'mp')
The draws below stay inside these ranges and needn't reach their ends.
Inputs may be any that keep to these rules, and one draw needn't show every extreme that they name: `seq_starts`: slot s lies in the buffer of dp index s // 8; the slots of one buffer are disjoint and in increasing order of start; start plus length is at most 1536, and in every draw the last slot of some buffer ends at row 1536. `episode_ids`: every class of every episode has at least one support sequence.
All inputs are finite; a program needn't handle non-finite values.
Results may differ from the reference program's by a relative error of at most 0.004.
Values sent between devices are 32-bit elements; how exact they have to be, the bound alone decides.
A program may use at most 128 MiB of HBM per device.

```python
import math
import jax
import jax.numpy as jnp
from jax import lax

D = 4096
HEAD_DIM = 128
HEADS = 16
KV_HEADS = 4
WAYS = 32
MIN_LEN = 128
SEQ_DEV = 8
CAP = 1536
NSEQ = 64
EPISODES = 1
CLASSES = 32


def packing(key):
    groups = NSEQ // SEQ_DEV
    subkeys = jax.random.split(jax.random.fold_in(key, 13), 4)
    spare_tokens = CAP - SEQ_DEV * MIN_LEN
    filled = jax.random.randint(subkeys[0], (groups,), 0, spare_tokens + 1)
    fullest = jax.random.randint(subkeys[1], (), 0, groups)
    filled = jnp.where(jnp.arange(groups) == fullest, spare_tokens, filled)
    raw_weights = jax.random.randint(subkeys[2], (groups, 2 * SEQ_DEV), 1, 17)
    weights = raw_weights * raw_weights * raw_weights
    shares = filled[:, None] * weights // jnp.sum(weights, axis=1, keepdims=True)
    remain = filled - jnp.sum(shares, axis=1)
    shares = shares.at[:, 0].add(remain)
    longest_slot = jax.random.randint(subkeys[3], (), 0, SEQ_DEV)
    single = jnp.where(jnp.arange(2 * SEQ_DEV) == longest_slot, spare_tokens, 0)
    shares = jnp.where((jnp.arange(groups) == fullest)[:, None], single[None, :], shares)
    lengths = MIN_LEN + shares[:, :SEQ_DEV]
    gap_sizes = shares[:, SEQ_DEV:]
    extents = lengths + gap_sizes
    starts = jnp.cumsum(extents, axis=1) - extents + gap_sizes
    return (starts.reshape(-1).astype(jnp.int32), lengths.reshape(-1).astype(jnp.int32))


def draw_seq_starts(key, part):
    return packing(key)[0]


def draw_seq_lengths(key, part):
    return packing(key)[1]


def labels(key):
    subkeys = jax.random.split(jax.random.fold_in(key, 7), 3)
    slot_index = jnp.arange(NSEQ, dtype=jnp.int32)
    extra_class = jax.random.randint(subkeys[0], (NSEQ,), 0, CLASSES)
    global_class = jnp.where(slot_index < CLASSES, slot_index, extra_class)
    coin = jax.random.randint(subkeys[1], (NSEQ,), 0, 2)
    asked_flag = jnp.where(slot_index < CLASSES, 0, jnp.where(slot_index == CLASSES, 1, coin))
    shuffle = jax.random.permutation(subkeys[2], NSEQ)
    return (global_class[shuffle], asked_flag[shuffle])


def draw_episode_ids(key, part):
    return (labels(key)[0] // WAYS).astype(jnp.int32)


def draw_class_ids(key, part):
    return (labels(key)[0] % WAYS).astype(jnp.int32)


def draw_query_flags(key, part):
    return labels(key)[1].astype(jnp.int32)


def query_key_pair(key):
    subkeys = jax.random.split(jax.random.fold_in(key, 21), 2)
    query_weight = jax.random.normal(subkeys[0], (D, HEADS * HEAD_DIM), jnp.float32) / math.sqrt(D)
    key_weight = jax.random.normal(subkeys[1], (D, KV_HEADS * HEAD_DIM), jnp.float32) / math.sqrt(D)
    return (jnp.clip(query_weight, -1.0, 1.0), jnp.clip(key_weight, -4.0, 4.0))


def draw_w_query(key, part):
    return query_key_pair(key)[0].astype(jnp.bfloat16)


def draw_w_key(key, part):
    return query_key_pair(key)[1].astype(jnp.bfloat16)


def draw_tokens(key, part):
    row_total = NSEQ // SEQ_DEV * CAP
    subkeys = jax.random.split(jax.random.fold_in(key, 31), 1)
    values = jax.random.normal(subkeys[0], (row_total, D), jnp.float32)
    values = jnp.clip(values, -6.0, 6.0)
    return values.astype(jnp.bfloat16)


def levels(own_key, shape, pieces, smallest, largest):
    level, own = 1.0, jax.random.fold_in(own_key, 6)
    for dim, parts in pieces:
        draws = jnp.exp(jax.random.uniform(jax.random.fold_in(own, dim), (parts,), jnp.float32, smallest / len(pieces), largest / len(pieces)))
        level = level * jnp.repeat(draws, shape[dim] // parts).reshape([-1 if axis == dim else 1 for axis in range(len(shape))])
    return level


def gaussian(key, shape, spread, most, shards=(), kind=jnp.bfloat16):
    entries = spread * jax.random.normal(key, shape, jnp.float32)
    if shards:
        entries = entries * levels(key, shape, shards, -0.22, 0.18)
    return jnp.clip(entries, -most, most).astype(kind)


def setup_inputs(seed: int = 0) -> dict:
    seeds = jax.random.split(jax.random.key(seed), 12)
    return {
        "tokens": draw_tokens(jax.random.fold_in(seeds[11], 71), 0),
        "norm_gain": jnp.clip(1.0 + 0.18 * jax.random.normal(seeds[1], (D,), jnp.float32), 0.099609375, 1.8984375).astype(jnp.bfloat16),
        "w_query": draw_w_query(jax.random.fold_in(seeds[11], 71), 0),
        "w_key": draw_w_key(jax.random.fold_in(seeds[11], 71), 0),
        "w_value": gaussian(seeds[4], (D, KV_HEADS * HEAD_DIM), D ** -0.5, 0.09375, ((1, 4),)),
        "w_out": gaussian(seeds[5], (HEADS * HEAD_DIM, D), (HEADS * HEAD_DIM) ** -0.5, 0.125, ((0, 4),)),
        "seq_starts": draw_seq_starts(jax.random.fold_in(seeds[11], 71), 0),
        "seq_lengths": draw_seq_lengths(jax.random.fold_in(seeds[11], 71), 0),
        "episode_ids": draw_episode_ids(jax.random.fold_in(seeds[11], 71), 0),
        "class_ids": draw_class_ids(jax.random.fold_in(seeds[11], 71), 0),
        "query_flags": draw_query_flags(jax.random.fold_in(seeds[11], 71), 0),
    }


ROPE_BASE = 500000.0
NEG_FILL = -1e+30

def rotate(vectors, positions):
    half_dim = vectors.shape[-1] // 2
    frequency = jnp.power(ROPE_BASE, -(jnp.arange(half_dim, dtype=jnp.float32) * 2.0 / vectors.shape[-1]))
    angles = positions.astype(jnp.float32)[:, None] * frequency[None, :]
    cosine = jnp.cos(angles)[:, None, :]
    sine_part = jnp.sin(angles)[:, None, :]
    leading = vectors[..., :half_dim]
    trailing = vectors[..., half_dim:]
    return jnp.concatenate([leading * cosine - trailing * sine_part, trailing * cosine + leading * sine_part], axis=-1)

def layout_of(starts, lengths, buffer_len):
    token_index = jnp.arange(buffer_len, dtype=jnp.int32)
    inside = (token_index[:, None] >= starts[None, :]) & (token_index[:, None] < (starts + lengths)[None, :])
    slot_number = jnp.arange(starts.shape[0], dtype=jnp.int32)
    segment = lax.optimization_barrier(jnp.sum(jnp.where(inside, slot_number[None, :] + 1, 0), axis=1)).astype(jnp.int32) - 1
    position = lax.optimization_barrier(jnp.sum(jnp.where(inside, token_index[:, None] - starts[None, :], 0), axis=1)).astype(jnp.int32)
    return (segment, position, inside)

def allowed_mask(segment, row_start, row_count, col_count):
    rows_index = row_start + jnp.arange(row_count, dtype=jnp.int32)
    cols_index = jnp.arange(col_count, dtype=jnp.int32)
    seg_rows = segment[row_start:row_start + row_count]
    seg_cols = segment[:col_count]
    same = (seg_rows[:, None] == seg_cols[None, :]) & (seg_rows[:, None] >= 0) & (cols_index[None, :] < rows_index[:, None])
    return (rows_index[:, None] == cols_index[None, :]) | same

def softmax_rows(scores, permitted):
    masked_scores = jnp.where(permitted[None, None], scores, NEG_FILL)
    row_peak = lax.optimization_barrier(jnp.max(masked_scores, axis=-1, keepdims=True))
    exponent = jnp.exp(masked_scores - row_peak)
    totals = lax.optimization_barrier(jnp.sum(exponent, axis=-1, keepdims=True))
    return (exponent / totals).astype(jnp.bfloat16)

def reference(tokens, norm_gain, w_query, w_key, w_value, w_out, seq_starts, seq_lengths, episode_ids, class_ids, query_flags):
    group_count = NSEQ // SEQ_DEV
    group_size = HEADS // KV_HEADS
    inv_root = 1.0 / math.sqrt(HEAD_DIM)
    highest = lax.Precision.HIGHEST

    def embed_group(row_items):
        buffer_rows, starts, lengths = row_items
        segment, position, inside = layout_of(starts, lengths, CAP)
        widened = buffer_rows.astype(jnp.float32)
        normed = (widened * lax.rsqrt(lax.optimization_barrier(jnp.mean(widened * widened, axis=-1, keepdims=True)) + 1e-05) * norm_gain.astype(jnp.float32)).astype(jnp.bfloat16)
        queries = rotate(jnp.dot(normed, w_query, preferred_element_type=jnp.float32).reshape(CAP, HEADS, HEAD_DIM), position).astype(jnp.bfloat16)
        queries = queries.reshape(CAP, KV_HEADS, group_size, HEAD_DIM)
        keys_rot = rotate(jnp.dot(normed, w_key, preferred_element_type=jnp.float32).reshape(CAP, KV_HEADS, HEAD_DIM), position).astype(jnp.bfloat16)
        values_all = jnp.dot(normed, w_value, preferred_element_type=jnp.float32).astype(jnp.bfloat16).reshape(CAP, KV_HEADS, HEAD_DIM)
        scores = jnp.einsum('qngd,knd->ngqk', queries.astype(jnp.float32), keys_rot.astype(jnp.float32), precision=highest) * inv_root
        permitted = allowed_mask(segment, 0, CAP, CAP)
        attention_probs = softmax_rows(scores, permitted)
        attended = jnp.einsum('ngqk,knd->qngd', attention_probs.astype(jnp.float32), values_all.astype(jnp.float32), precision=highest)
        attended = attended.astype(jnp.bfloat16).reshape(CAP, HEADS * HEAD_DIM)
        layer_out = widened + jnp.dot(attended, w_out, preferred_element_type=jnp.float32)
        member = inside.T.astype(jnp.float32)
        return jnp.dot(member, layer_out, precision=highest) / lengths.astype(jnp.float32)[:, None]
    pooled = lax.map(embed_group, (tokens.reshape(group_count, CAP, D), seq_starts.reshape(group_count, SEQ_DEV), seq_lengths.reshape(group_count, SEQ_DEV)))
    pooled = pooled.reshape(NSEQ, D)
    embedded = pooled * lax.rsqrt(lax.optimization_barrier(jnp.mean(pooled * pooled, axis=-1, keepdims=True)) + 1e-06)
    global_class = episode_ids * WAYS + class_ids
    is_support = query_flags == 0
    select_all = ((global_class[None, :] == jnp.arange(CLASSES, dtype=jnp.int32)[:, None]) & is_support[None, :]).astype(jnp.float32)
    class_sums = jnp.dot(select_all, embedded, precision=highest)
    prototypes = class_sums * lax.rsqrt(lax.optimization_barrier(jnp.mean(class_sums * class_sums, axis=-1, keepdims=True)) + 1e-06)
    episode_protos = prototypes.reshape(EPISODES, WAYS, D)

    def score_row(row_items):
        vector, episode = row_items
        chosen = lax.dynamic_index_in_dim(episode_protos, episode, 0, keepdims=False)
        difference = vector[None, :] - chosen
        return lax.optimization_barrier(jnp.sum(difference * difference, axis=-1))
    distance = lax.map(score_row, (embedded, episode_ids))
    logits = -distance / math.sqrt(D)
    row_peak = lax.optimization_barrier(jnp.max(logits, axis=-1, keepdims=True))
    shifted = logits - row_peak
    log_probs = shifted - jnp.log(lax.optimization_barrier(jnp.sum(jnp.exp(shifted), axis=-1, keepdims=True)))
    log_probs = jnp.where(query_flags[:, None] == 1, log_probs, 0.0)
    return (log_probs, prototypes)
```

```python
import functools
import math

import numpy as np
import jax
import jax.numpy as jnp
from jax import lax
from jax.experimental import pallas as pl
from jax.experimental.pallas import tpu as pltpu
from jax.sharding import PartitionSpec as P

HEAD_DIM = 128
WAYS = 32
ROPE_BASE = 500000.0
NEG_FILL = -1e30
MAX_LEN = 640
MIN_LEN = 128
QB = 128
MESH = pl.DeviceIdType.MESH
F32 = jnp.float32
BF16 = jnp.bfloat16
HIGHEST = lax.Precision.HIGHEST


def pick(total, options):
    for candidate in options:
        if total % candidate == 0:
            return candidate
    return total


def fused_kernel(
    dims, st_hbm, ln_hbm, gain_hbm, ep_hbm, cl_hbm, fl_hbm,
    x_hbm, wq_hbm, wk_hbm, wv_hbm, wo_hbm, trig_hbm,
    lp_ref, pr_ref, x_s, xg_s, w_s, wo_s, trig_s, qt_s, k_s, v_s, e_s, c_s, p_s, mx_s, ts_s,
    hp_s, rs_s, ag_s, ga_s, gb_s, st_ref, ln_ref, gain_ref, ep_ref, cl_ref, fl_ref,
    few_sem, x_sem, head_sem, w_sem, wo_sem, trig_sem,
    rs_send, rs_recv, ag_send, ag_recv, g_send, g_recv,
):
    rows, tile, width, slots, heads, chunk, share, n_mp, n_dp, classes = dims
    hd = HEAD_DIM
    i = pl.program_id(0)
    tiles = rows // tile
    q_cols = heads * hd
    chunks = width // chunk
    blocks = tile // QB
    slack = rows - MIN_LEN * slots

    def lowest(qb):
        first = qb * QB
        start = max(0, first - MAX_LEN + 1, MIN_LEN * ((first - slack) // MIN_LEN))
        return start // QB

    few = [
        pltpu.make_async_copy(src, dst, few_sem.at[k])
        for k, (src, dst) in enumerate((
            (gain_hbm, gain_ref), (st_hbm, st_ref), (ln_hbm, ln_ref),
            (ep_hbm, ep_ref), (cl_hbm, cl_ref), (fl_hbm, fl_ref),
        ))
    ]

    def head_copy(c):
        at = (pl.ds(0, tile), pl.ds(c * chunk, chunk))
        return pltpu.make_async_copy(x_hbm.at[at], x_s.at[at], head_sem.at[c])

    half = slots // 2
    near = n_dp * half
    dp = lax.axis_index("dp")
    rank = lax.axis_index("mp")
    wo_copy = pltpu.make_async_copy(wo_hbm, wo_s, wo_sem)
    trig_copy = pltpu.make_async_copy(trig_hbm, trig_s, trig_sem)

    def x_copy(t):
        r = pl.ds(t * tile, tile)
        return pltpu.make_async_copy(x_hbm.at[r, :], x_s.at[r, :], x_sem.at[t])

    def w_copies(c):
        r = pl.ds(c * chunk, chunk)
        return (
            pltpu.make_async_copy(wq_hbm.at[r, :], w_s.at[r, pl.ds(0, q_cols)], w_sem.at[c, 0]),
            pltpu.make_async_copy(wk_hbm.at[r, :], w_s.at[r, pl.ds(q_cols, hd)], w_sem.at[c, 1]),
            pltpu.make_async_copy(wv_hbm.at[r, :], w_s.at[r, pl.ds(q_cols + hd, hd)], w_sem.at[c, 2]),
        )

    def members(first, count):
        slot = lax.broadcasted_iota(jnp.int32, (slots, count), 0)
        token = lax.broadcasted_iota(jnp.int32, (slots, count), 1) + first
        lo = jnp.zeros((slots, count), jnp.int32)
        hi = jnp.zeros((slots, count), jnp.int32)
        for j in range(slots):
            lo = jnp.where(slot == j, st_ref[j], lo)
            hi = jnp.where(slot == j, st_ref[j] + ln_ref[j], hi)
        return jnp.where((token >= lo) & (token < hi), 1.0, 0.0).astype(BF16)

    def project(t):
        r0 = t * tile
        sums = [jnp.zeros((QB, 256), F32) for _ in range(blocks)]

        def scale(c):
            for b in range(blocks):
                r = slice(r0 + b * QB, r0 + (b + 1) * QB)
                for v in range(c * chunk, (c + 1) * chunk, 1024):
                    pair = []
                    for u in range(v, v + 1024, 256):
                        x = x_s[r, u : u + 256]
                        xg_s[b * QB : (b + 1) * QB, u : u + 256] = x * gain_ref[u : u + 256][None, :]
                        pair.append(x * x)
                    sums[b] = sums[b] + ((pair[0] + pair[1]) + (pair[2] + pair[3])).astype(F32)

        scale(0)
        for c in range(chunks):
            if t == 0:
                with jax.named_scope(f"wwait{c}"):
                    for copy in w_copies(c):
                        copy.wait()
                    if c + 1 < chunks:
                        head_copy(c + 1).wait()
                if c + 2 < chunks:
                    for copy in w_copies(c + 2):
                        copy.start()
                    if c + 3 < chunks:
                        head_copy(c + 3).start()
                if c + 2 == chunks - 1:
                    trig_copy.start()
                    x_copy(1).start()
            s = slice(c * chunk, (c + 1) * chunk)
            part = jnp.dot(xg_s[:, s], w_s[s, :], preferred_element_type=F32)
            p_s[...] = part if c == 0 else p_s[...] + part
            if c + 1 < chunks:
                scale(c + 1)
            yield
        if t == 0:
            trig_copy.wait()
            for copy in few[1:]:
                copy.wait()
        stats = [jnp.sum(a, axis=-1, keepdims=True) for a in sums]
        rstd = lax.rsqrt(jnp.concatenate(stats, axis=0) / width + 1e-05)
        cols = pl.ds(pl.multiple_of(rank * share, share), share)
        ts = jnp.dot(members(r0, tile), x_s[r0 : r0 + tile, cols], preferred_element_type=F32)
        if t == 0:
            ts_s[...] = ts
        else:
            ts_s[...] += ts
        trig = trig_s[r0 : r0 + tile, :]
        turned = pltpu.roll(trig, hd // 2, 1)
        front = lax.broadcasted_iota(jnp.int32, (tile, hd), 1) < hd // 2
        cos = jnp.where(front, trig, turned)
        sin = jnp.where(front, -turned, trig)

        def rope(y):
            return y * cos + pltpu.roll(y, hd // 2, 1) * sin

        q_rstd = rstd * (math.log2(math.e) / math.sqrt(hd))
        for h in range(heads):
            q = rope(p_s[:, h * hd : (h + 1) * hd] * q_rstd)
            for b in range(blocks):
                qt_s[t % 2, b, :, h * QB : (h + 1) * QB] = q[b * QB : (b + 1) * QB].T.astype(BF16)
        k_s[r0 : r0 + tile, :] = rope(p_s[:, q_cols : q_cols + hd] * rstd).astype(BF16)
        v_s[r0 : r0 + tile, :] = (p_s[:, q_cols + hd :] * rstd).astype(BF16)

    def mix(kb, h, part):
        r = slice(kb * QB, (kb + 1) * QB)
        mass = jnp.sum(part, axis=-1, keepdims=True)
        mx_s[r, h * hd : (h + 1) * hd] = (mass * v_s[r, :].astype(F32)).astype(BF16)

    def attend(t, mixed):
        scales = {}
        for b in range(blocks):
            qb = t * blocks + b
            first = qb * QB
            token = lax.broadcasted_iota(jnp.int32, (1, QB), 1) + first
            start = token
            for j in range(slots):
                s0 = st_ref[j]
                start = jnp.where((token >= s0) & (token < s0 + ln_ref[j]), s0, start)
            low = lowest(qb)
            peaks = {}
            totals = {}
            for kb in range(low, qb + 1):
                s_all = jnp.dot(
                    k_s[kb * QB : (kb + 1) * QB, :], qt_s[t % 2, b], preferred_element_type=F32
                )
                row = lax.broadcasted_iota(jnp.int32, (QB, QB), 0) + kb * QB
                ok = row >= start
                if kb == qb:
                    ok = ok & (row <= token)
                for h in range(heads):
                    s = jnp.where(ok, s_all[:, h * QB : (h + 1) * QB], NEG_FILL)
                    s = s.reshape(QB // 8, 8, QB)
                    peak = jnp.max(s, axis=0)
                    e = jnp.exp2(s - peak[None])
                    e_s[b, kb - low, h] = e.reshape(QB, QB)
                    peaks[kb, h] = peak
                    totals[kb, h] = jnp.sum(e, axis=0)
            for h in range(heads):
                top = peaks[low, h]
                for kb in range(low + 1, qb + 1):
                    top = jnp.maximum(top, peaks[kb, h])
                top = jnp.max(top, axis=0, keepdims=True)
                total = jnp.zeros((8, QB), F32)
                gain = {}
                for kb in range(low, qb + 1):
                    gain[kb] = jnp.exp2(peaks[kb, h] - top)
                    total = total + gain[kb] * totals[kb, h]
                inverse = 1.0 / jnp.sum(total, axis=0, keepdims=True)
                for kb in range(low, qb + 1):
                    scales[b, kb, h] = gain[kb] * inverse
            yield
        low0 = lowest(t * blocks)
        end0 = (t + 1) * blocks
        if mixed is not None:
            for kb in range(mixed, low0):
                for h in range(heads):
                    mix(kb, h, c_s[h, kb * QB : (kb + 1) * QB, :])
        for kb in range(low0, end0):
            if kb == (low0 + end0) // 2:
                yield
            for h in range(heads):
                r = slice(kb * QB, (kb + 1) * QB)
                part = None if kb >= t * blocks else c_s[h, r, :].reshape(QB // 8, 8, QB)
                for b in range(blocks):
                    if (b, kb, h) in scales:
                        low = lowest(t * blocks + b)
                        e = e_s[b, kb - low, h].reshape(QB // 8, 8, QB) * scales[b, kb, h][None]
                        part = e if part is None else part + e
                part = part.reshape(QB, QB)
                c_s[h, r, :] = part
                if mixed is not None and kb >= mixed:
                    mix(kb, h, part)

    bound = (rows - MIN_LEN * (slots - half), rows)
    floor = (0, MIN_LEN * half // QB)
    ready = (-(-bound[0] // tile) - 1, tiles - 1)

    def finish(p):
        low, high = floor[p] * QB, (ready[p] + 1) * tile
        attended = jnp.dot(
            members(low, high - low), mx_s[low:high, :], preferred_element_type=F32
        )
        upper = attended.astype(BF16)
        lower = attended - upper.astype(F32)
        both = jnp.concatenate([upper.astype(F32), lower], axis=0).astype(BF16)
        for m in range(n_mp):
            out = jnp.dot(both, wo_s[:, m * share : (m + 1) * share], preferred_element_type=F32)
            out = out[:slots] + out[slots:]
            hp_s[p, m] = out[p * half : (p + 1) * half]
            if m == n_mp // 2 - 1:
                yield

    def signal_all():
        barrier = pltpu.get_barrier_semaphore()
        for d in range(1, n_mp):
            peer = (dp, lax.rem(rank + d, n_mp))
            pl.semaphore_signal(barrier, inc=1, device_id=peer, device_id_type=MESH)
        for d in range(1, n_dp):
            peer = (lax.rem(dp + d, n_dp), rank)
            pl.semaphore_signal(barrier, inc=1, device_id=peer, device_id_type=MESH)

    def rs_copy(p, d):
        peer = lax.rem(rank + d, n_mp)
        return pltpu.make_async_remote_copy(
            src_ref=hp_s.at[p, peer], dst_ref=rs_s.at[p, d - 1],
            send_sem=rs_send.at[p, d - 1], recv_sem=rs_recv.at[p, d - 1],
            device_id=(dp, peer), device_id_type=MESH,
        )

    def ag_copy(p, d):
        return pltpu.make_async_remote_copy(
            src_ref=ag_s.at[p, dp], dst_ref=ag_s.at[p, dp],
            send_sem=ag_send.at[p, d - 1], recv_sem=ag_recv.at[p, d - 1],
            device_id=(lax.rem(dp + d, n_dp), rank), device_id_type=MESH,
        )

    def g_copy(p, d):
        ref = (ga_s, gb_s)[p]
        return pltpu.make_async_remote_copy(
            src_ref=ref.at[rank], dst_ref=ref.at[rank],
            send_sem=g_send.at[p, d - 1], recv_sem=g_recv.at[p, d - 1],
            device_id=(dp, lax.rem(rank + d, n_mp)), device_id_type=MESH,
        )

    def pool(p):
        with jax.named_scope(f"rs{p}"):
            for d in range(1, n_mp):
                rs_copy(p, d).wait_recv()
        slot = lax.broadcasted_iota(jnp.int32, (half, share), 0)
        count = jnp.ones((half, share), F32)
        for j in range(half):
            count = jnp.where(slot == j, ln_ref[p * half + j].astype(F32), count)
        pooled = ts_s[p * half : (p + 1) * half, :] + hp_s[p, rank]
        for d in range(1, n_mp):
            pooled = pooled + rs_s[p, d - 1]
        ag_s[p, dp] = pooled / count
        for d in range(1, n_dp):
            ag_copy(p, d).start()

    def split(a):
        upper = a.astype(BF16)
        return upper, (a - upper.astype(F32)).astype(BF16)

    def product(a, b, axes):
        (ah, al), (bh, bl) = a, b
        where = ((axes[:1], axes[1:]), ((), ()))
        def one(u, w):
            return lax.dot_general(u, w, where, preferred_element_type=F32)
        if al is None:
            return one(ah, bh) + one(ah, bl)
        return one(ah, bh) + (one(ah, bl) + one(al, bh))

    def gathered(p):
        with jax.named_scope(f"ag{p}"):
            for d in range(1, n_dp):
                ag_copy(p, d).wait_recv()
        return split(jnp.concatenate([ag_s[p, d] for d in range(n_dp)], axis=0))

    def folded(a):
        f = max(1, 128 // a.shape[1])
        tall = a.shape[0] // f
        return jnp.concatenate([a[k * tall : (k + 1) * tall] for k in range(f)], axis=1)

    def unfolded(ref, columns):
        total = ref[0]
        for m in range(1, n_mp):
            total = total + ref[m]
        f = total.shape[1] // columns
        return jnp.concatenate(
            [total[:, k * columns : (k + 1) * columns] for k in range(f)], axis=0
        )

    def tail():
        nseq = 2 * near
        for d in range(1, n_mp):
            rs_copy(1, d).start()
        pool(0)
        pool(1)
        place = lax.broadcasted_iota(jnp.int32, (nseq, nseq), 1)
        spot = place % near
        origin = (spot // half) * slots + (place // near) * half + spot % half
        order = jnp.where(
            lax.broadcasted_iota(jnp.int32, (nseq, nseq), 0) == origin, 1.0, 0.0
        ).astype(BF16)
        facts = jnp.concatenate(
            [ref[...].astype(F32).reshape(1, nseq) for ref in (ep_ref, cl_ref, fl_ref)]
            + [jnp.zeros((5, nseq), F32)], axis=0,
        ).astype(BF16)
        facts = jnp.dot(facts, order, preferred_element_type=F32)
        episode, label, query = facts[0:1], facts[1:2], facts[2:3]
        label = episode * float(WAYS) + label
        class_row = lax.broadcasted_iota(jnp.int32, (classes, nseq), 0).astype(F32)
        select = jnp.where((class_row == label) & (query == 0.0), 1.0, 0.0)
        a = lax.broadcasted_iota(jnp.int32, (slots, nseq), 0)
        a = (a // half) * near + dp * half + a % half
        mine = a == lax.broadcasted_iota(jnp.int32, (slots, nseq), 1)
        own_query = jnp.sum(jnp.where(mine, query, 0.0), axis=-1, keepdims=True)
        own_episode = jnp.sum(jnp.where(mine, episode, 0.0), axis=-1, keepdims=True)
        eye = lax.broadcasted_iota(jnp.int32, (nseq, nseq), 0) == lax.broadcasted_iota(
            jnp.int32, (nseq, nseq), 1
        )
        eye_c = lax.broadcasted_iota(jnp.int32, (classes, classes), 0) == lax.broadcasted_iota(
            jnp.int32, (classes, classes), 1
        )
        x0 = gathered(0)
        ga_s[rank] = folded(product(x0, x0, (1, 1)))
        for d in range(1, n_mp):
            g_copy(0, d).start()
        x1 = gathered(1)
        gb_s[rank] = folded(
            jnp.concatenate([product(x1, x0, (1, 1)), product(x1, x1, (1, 1))], axis=1)
        )
        for d in range(1, n_mp):
            g_copy(1, d).start()
        every = tuple(jnp.concatenate([u, w], axis=0) for u, w in zip(x0, x1))
        for p in range(2):
            for d in range(1, n_mp):
                rs_copy(p, d).wait_send()
            for d in range(1, n_dp):
                ag_copy(p, d).wait_send()
        with jax.named_scope("gwait"):
            for p in range(2):
                for d in range(1, n_mp):
                    g_copy(p, d).wait_recv()
        with jax.named_scope("score"):
            score(select, every, mine, eye, eye_c, own_query, own_episode)
        for p in range(2):
            for d in range(1, n_mp):
                g_copy(p, d).wait_send()

    def score(select, every, mine, eye, eye_c, own_query, own_episode):
        nseq = 2 * near
        g00 = unfolded(ga_s, near)
        below = unfolded(gb_s, nseq)
        gram = jnp.concatenate(
            [jnp.concatenate([g00, below[:, :near].T], axis=1), below], axis=0
        )
        diag = jnp.where(eye, gram, 0.0)
        norms = jnp.sum(diag, axis=0, keepdims=True)
        scale_row = lax.rsqrt(norms / width + 1e-06)
        norms = norms * scale_row * scale_row
        scale_col = lax.rsqrt(jnp.sum(diag, axis=1, keepdims=True) / width + 1e-06)
        gram = gram * scale_row * scale_col
        cross_t = product((select.astype(BF16), None), split(gram), (1, 0))
        norm_col = jnp.maximum(jnp.sum(cross_t * select, axis=1, keepdims=True), 0.0)
        proto_col = lax.rsqrt(norm_col / width + 1e-06)
        pr_ref[...] = product(split(select * scale_row), every, (1, 0)) * proto_col
        cross = product((mine.astype(F32).astype(BF16), None), split(cross_t), (1, 1))
        norm_row = jnp.sum(jnp.where(eye_c, norm_col, 0.0), axis=0, keepdims=True)
        proto_row = lax.rsqrt(norm_row / width + 1e-06)
        own_norm = jnp.sum(jnp.where(mine, norms, 0.0), axis=-1, keepdims=True)
        distance = own_norm - 2.0 * (cross * proto_row) + norm_row * proto_row * proto_row
        picked = jnp.zeros((slots, WAYS), F32)
        for e in range(classes // WAYS):
            picked = jnp.where(own_episode == float(e), distance[:, e * WAYS : (e + 1) * WAYS], picked)
        logits = -picked / math.sqrt(width)
        shifted = logits - jnp.max(logits, axis=-1, keepdims=True)
        logp = shifted - jnp.log(jnp.sum(jnp.exp(shifted), axis=-1, keepdims=True))
        lp_ref[...] = jnp.where(own_query == 1.0, logp, 0.0)

    for step in range(tiles + 1):
        @pl.when(i == step)
        def _(step=step):
            if step == 0:
                head_copy(0).start()
                few[0].start()
                for c in range(min(2, chunks)):
                    if c + 1 < chunks:
                        head_copy(c + 1).start()
                    for copy in w_copies(c):
                        copy.start()
                for copy in few[1:]:
                    copy.start()
                signal_all()
            if 0 < step < tiles - 1:
                x_copy(step + 1).start()
            if step == 2:
                wo_copy.start()
            if step < tiles:
                with jax.named_scope("xwait"):
                    if step == 0:
                        few[0].wait()
                        head_copy(0).wait()
                    else:
                        x_copy(step).wait()
            if step == ready[0] + 2:
                wo_copy.wait()
            with jax.named_scope(f"step{step}"):
                work = []
                if step < tiles:
                    work.append(project(step))
                if step == ready[0] + 2:
                    work.append(finish(0))
                if step > 0:
                    mixed = [floor[p] for p in range(2) if ready[p] == step - 1]
                    work.append(attend(step - 1, mixed[0] if mixed else None))
                while work:
                    work = [w for w in work if next(w, True) is None]
            if step == ready[0] + 2:
                with jax.named_scope("barrier"):
                    pl.semaphore_wait(pltpu.get_barrier_semaphore(), n_mp + n_dp - 2)
                for d in range(1, n_mp):
                    rs_copy(0, d).start()
            if step == tiles:
                with jax.named_scope("finish"):
                    for _ in finish(1):
                        pass
                with jax.named_scope("tail"):
                    tail()


def copy_kernel(a_ref, b_ref, x_ref, y_ref):
    x_ref[...] = a_ref[...]
    y_ref[...] = b_ref[...]


def per_device(
    n_dp, n_mp, tokens, norm_gain, w_query, w_key, w_value, w_out,
    seq_starts, seq_lengths, episode_ids, class_ids, query_flags,
):
    rows, width = tokens.shape
    slots = seq_starts.shape[0]
    hd = HEAD_DIM
    heads = w_query.shape[1] // hd
    assert w_key.shape[1] == hd
    share = width // n_mp
    tile = pick(rows, (256, 128))
    chunk = pick(width, (1024, 512, 256, 128))
    frequency = ROPE_BASE ** (-np.arange(hd // 2, dtype=np.float64) * 2.0 / hd)
    angles = np.arange(rows, dtype=np.float64)[:, None] * frequency[None, :]
    trig = jnp.asarray(np.concatenate([np.cos(angles), np.sin(angles)], axis=1), F32)
    vmem = pl.BlockSpec(memory_space=pltpu.VMEM)
    hbm = pl.BlockSpec(memory_space=pl.ANY)
    nseq = episode_ids.shape[0]
    classes = max(1, nseq // (2 * WAYS)) * WAYS
    half = slots // 2
    near = n_dp * half
    fold_a = max(1, 128 // near)
    fold_b = max(1, 128 // nseq)
    span = -(-(MAX_LEN - 1) // QB) + 1
    dma = pltpu.SemaphoreType.DMA
    dims = (rows, tile, width, slots, heads, chunk, share, n_mp, n_dp, classes)
    outs = pl.pallas_call(
        functools.partial(fused_kernel, dims),
        grid=(rows // tile + 1,),
        out_shape=(
            jax.ShapeDtypeStruct((slots, WAYS), F32),
            jax.ShapeDtypeStruct((classes, share), F32),
        ),
        in_specs=[hbm] * 12,
        out_specs=(
            pl.BlockSpec((slots, WAYS), lambda i: (0, 0)),
            pl.BlockSpec((classes, share), lambda i: (0, 0)),
        ),
        scratch_shapes=[
            pltpu.VMEM((rows, width), BF16),
            pltpu.VMEM((tile, width), BF16),
            pltpu.VMEM((width, (heads + 2) * hd), BF16),
            pltpu.VMEM(w_out.shape, BF16),
            pltpu.VMEM((rows, hd), F32),
            pltpu.VMEM((2, tile // QB, hd, heads * QB), BF16),
            pltpu.VMEM((rows, hd), BF16),
            pltpu.VMEM((rows, hd), BF16),
            pltpu.VMEM((tile // QB, span, heads, QB, QB), F32),
            pltpu.VMEM((heads, rows, QB), F32),
            pltpu.VMEM((tile, (heads + 2) * hd), F32),
            pltpu.VMEM((rows, heads * hd), BF16),
            pltpu.VMEM((slots, share), F32),
            pltpu.VMEM((2, n_mp, half, share), F32),
            pltpu.VMEM((2, n_mp - 1, half, share), F32),
            pltpu.VMEM((2, n_dp, half, share), F32),
            pltpu.VMEM((n_mp, near // fold_a, near * fold_a), F32),
            pltpu.VMEM((n_mp, near // fold_b, nseq * fold_b), F32),
            pltpu.SMEM((slots,), jnp.int32),
            pltpu.SMEM((slots,), jnp.int32),
            pltpu.VMEM((width,), BF16),
            pltpu.VMEM((nseq,), jnp.int32),
            pltpu.VMEM((nseq,), jnp.int32),
            pltpu.VMEM((nseq,), jnp.int32),
            dma((6,)),
            dma((rows // tile,)),
            dma((width // chunk,)),
            dma((width // chunk, 3)),
            dma,
            dma,
            dma((2, n_mp - 1)), dma((2, n_mp - 1)),
            dma((2, n_dp - 1)), dma((2, n_dp - 1)),
            dma((2, n_mp - 1)), dma((2, n_mp - 1)),
        ],
        compiler_params=pltpu.CompilerParams(
            dimension_semantics=("arbitrary",), vmem_limit_bytes=60 * 1024 * 1024,
            collective_id=0, has_side_effects=True,
        ),
    )(
        seq_starts, seq_lengths, norm_gain,
        episode_ids, class_ids, query_flags,
        tokens, w_query, w_key, w_value, w_out, trig,
    )
    return pl.pallas_call(
        copy_kernel,
        out_shape=tuple(jax.ShapeDtypeStruct(a.shape, a.dtype) for a in outs),
        in_specs=[vmem, vmem],
        out_specs=(vmem, vmem),
    )(*outs)


def solution(mesh):
    placed = (
        P("dp", None), P(), P(None, "mp"), P(None, "mp"), P(None, "mp"), P("mp", None),
        P("dp"), P("dp"), P(), P(), P(),
    )
    return jax.shard_map(
        functools.partial(per_device, mesh.shape["dp"], mesh.shape["mp"]),
        mesh=mesh,
        in_specs=placed,
        out_specs=(P("dp", None), P(None, "mp")),
        check_vma=False,
    )
```

```python
import functools
import math

import numpy as np
import jax
import jax.numpy as jnp
from jax import lax
from jax.experimental import pallas as pl
from jax.experimental.pallas import tpu as pltpu
from jax.sharding import PartitionSpec as P

HEAD_DIM = 128
WAYS = 32
ROPE_BASE = 500000.0
NEG_FILL = -1e30
MAX_LEN = 640
MIN_LEN = 128
QB = 128
MESH = pl.DeviceIdType.MESH
F32 = jnp.float32
BF16 = jnp.bfloat16
HIGHEST = lax.Precision.HIGHEST


def pick(total, options):
    for candidate in options:
        if total % candidate == 0:
            return candidate
    return total


def fused_kernel(
    dims, st_hbm, ln_hbm, gain_hbm, ep_hbm, cl_hbm, fl_hbm,
    x_hbm, wq_hbm, wk_hbm, wv_hbm, wo_hbm, trig_hbm,
    lp_ref, pr_ref, x_s, xg_s, w_s, wo_s, trig_s, qt_s, k_s, v_s, e_s, c_s, p_s, mx_s, ts_s,
    hp_s, rs_s, ag_s, ga_s, gb_s, st_ref, ln_ref, gain_ref, ep_ref, cl_ref, fl_ref,
    few_sem, x_sem, head_sem, w_sem, wo_sem, trig_sem,
    rs_send, rs_recv, ag_send, ag_recv, g_send, g_recv,
):
    rows, tile, width, slots, heads, chunk, piece, share, n_mp, n_dp, classes = dims
    hd = HEAD_DIM
    i = pl.program_id(0)
    tiles = rows // tile
    q_cols = heads * hd
    chunks = width // chunk
    blocks = tile // QB
    slack = rows - MIN_LEN * slots

    def lowest(qb):
        first = qb * QB
        start = max(0, first - MAX_LEN + 1, MIN_LEN * ((first - slack) // MIN_LEN))
        return start // QB

    few = [
        pltpu.make_async_copy(src, dst, few_sem.at[k])
        for k, (src, dst) in enumerate((
            (gain_hbm, gain_ref), (st_hbm, st_ref), (ln_hbm, ln_ref),
            (ep_hbm, ep_ref), (cl_hbm, cl_ref), (fl_hbm, fl_ref),
        ))
    ]

    def head_copy(c):
        at = (pl.ds(0, tile), pl.ds(c * chunk, chunk))
        return pltpu.make_async_copy(x_hbm.at[at], x_s.at[at], head_sem.at[c])

    half = slots // 2
    near = n_dp * half
    dp = lax.axis_index("dp")
    rank = lax.axis_index("mp")
    wo_copy = pltpu.make_async_copy(wo_hbm, wo_s, wo_sem)
    trig_copy = pltpu.make_async_copy(trig_hbm, trig_s, trig_sem)

    def x_copy(t):
        r = pl.ds(t * tile, tile)
        return pltpu.make_async_copy(x_hbm.at[r, :], x_s.at[r, :], x_sem.at[t])

    def w_copies(c):
        r = pl.ds(c * chunk, chunk)
        return (
            pltpu.make_async_copy(wq_hbm.at[r, :], w_s.at[r, pl.ds(0, q_cols)], w_sem.at[c, 0]),
            pltpu.make_async_copy(wk_hbm.at[r, :], w_s.at[r, pl.ds(q_cols, hd)], w_sem.at[c, 1]),
            pltpu.make_async_copy(wv_hbm.at[r, :], w_s.at[r, pl.ds(q_cols + hd, hd)], w_sem.at[c, 2]),
        )

    def members(first, count):
        slot = lax.broadcasted_iota(jnp.int32, (slots, count), 0)
        token = lax.broadcasted_iota(jnp.int32, (slots, count), 1) + first
        lo = jnp.zeros((slots, count), jnp.int32)
        hi = jnp.zeros((slots, count), jnp.int32)
        for j in range(slots):
            lo = jnp.where(slot == j, st_ref[j], lo)
            hi = jnp.where(slot == j, st_ref[j] + ln_ref[j], hi)
        return jnp.where((token >= lo) & (token < hi), 1.0, 0.0).astype(BF16)

    def project(t):
        r0 = t * tile
        span = chunk if t == 0 else piece
        count = width // span
        sums = [jnp.zeros((QB, 256), F32) for _ in range(blocks)]

        def scale(c):
            for b in range(blocks):
                r = slice(r0 + b * QB, r0 + (b + 1) * QB)
                for v in range(c * span, (c + 1) * span, 1024):
                    pair = []
                    for u in range(v, v + 1024, 256):
                        x = x_s[r, u : u + 256]
                        xg_s[b * QB : (b + 1) * QB, u : u + 256] = x * gain_ref[u : u + 256][None, :]
                        pair.append(x * x)
                    sums[b] = sums[b] + ((pair[0] + pair[1]) + (pair[2] + pair[3])).astype(F32)

        for c in range(count if t == 0 else 1):
            if t == 0 and c > 0:
                head_copy(c).wait()
            scale(c)
        for c in range(count):
            if t == 0:
                with jax.named_scope(f"wwait{c}"):
                    for copy in w_copies(c):
                        copy.wait()
                if 0 < c and c + 1 < chunks:
                    for copy in w_copies(c + 1):
                        copy.start()
                if c == max(0, chunks - 2):
                    trig_copy.start()
                    x_copy(1).start()
            s = slice(c * span, (c + 1) * span)
            part = jnp.dot(xg_s[:, s], w_s[s, :], preferred_element_type=F32)
            p_s[...] = part if c == 0 else p_s[...] + part
            if t > 0 and c + 1 < count:
                scale(c + 1)
            for _ in range(4 // count):
                yield
        if t == 0:
            trig_copy.wait()
            for copy in few[1:]:
                copy.wait()
        stats = [jnp.sum(a, axis=-1, keepdims=True) for a in sums]
        rstd = lax.rsqrt(jnp.concatenate(stats, axis=0) / width + 1e-05)
        cols = pl.ds(pl.multiple_of(rank * share, share), share)
        ts = jnp.dot(members(r0, tile), x_s[r0 : r0 + tile, cols], preferred_element_type=F32)
        if t == 0:
            ts_s[...] = ts
        else:
            ts_s[...] += ts
        trig = trig_s[r0 : r0 + tile, :]
        turned = pltpu.roll(trig, hd // 2, 1)
        front = lax.broadcasted_iota(jnp.int32, (tile, hd), 1) < hd // 2
        cos = jnp.where(front, trig, turned)
        sin = jnp.where(front, -turned, trig)

        def rope(y):
            return y * cos + pltpu.roll(y, hd // 2, 1) * sin

        q_rstd = rstd * (math.log2(math.e) / math.sqrt(hd))
        for h in range(heads):
            q = rope(p_s[:, h * hd : (h + 1) * hd] * q_rstd)
            for b in range(blocks):
                qt_s[t % 2, b, :, h * QB : (h + 1) * QB] = q[b * QB : (b + 1) * QB].T.astype(BF16)
        k_s[r0 : r0 + tile, :] = rope(p_s[:, q_cols : q_cols + hd] * rstd).astype(BF16)
        v_s[r0 : r0 + tile, :] = (p_s[:, q_cols + hd :] * rstd).astype(BF16)

    def mix(kb, h, part):
        r = slice(kb * QB, (kb + 1) * QB)
        mass = jnp.sum(part, axis=-1, keepdims=True)
        mx_s[r, h * hd : (h + 1) * hd] = (mass * v_s[r, :].astype(F32)).astype(BF16)

    def attend(t, mixed):
        scales = {}
        for b in range(blocks):
            qb = t * blocks + b
            first = qb * QB
            token = lax.broadcasted_iota(jnp.int32, (1, QB), 1) + first
            start = token
            for j in range(slots):
                s0 = st_ref[j]
                start = jnp.where((token >= s0) & (token < s0 + ln_ref[j]), s0, start)
            low = lowest(qb)
            peaks = {}
            totals = {}
            for kb in range(low, qb + 1):
                s_all = jnp.dot(
                    k_s[kb * QB : (kb + 1) * QB, :], qt_s[t % 2, b], preferred_element_type=F32
                )
                row = lax.broadcasted_iota(jnp.int32, (QB, QB), 0) + kb * QB
                ok = row >= start
                if kb == qb:
                    ok = ok & (row <= token)
                for h in range(heads):
                    s = jnp.where(ok, s_all[:, h * QB : (h + 1) * QB], NEG_FILL)
                    s = s.reshape(QB // 8, 8, QB)
                    peak = jnp.max(s, axis=0)
                    e = jnp.exp2(s - peak[None])
                    e_s[b, kb - low, h] = e.reshape(QB, QB)
                    peaks[kb, h] = peak
                    totals[kb, h] = jnp.sum(e, axis=0)
            for h in range(heads):
                top = peaks[low, h]
                for kb in range(low + 1, qb + 1):
                    top = jnp.maximum(top, peaks[kb, h])
                top = jnp.max(top, axis=0, keepdims=True)
                total = jnp.zeros((8, QB), F32)
                gain = {}
                for kb in range(low, qb + 1):
                    gain[kb] = jnp.exp2(peaks[kb, h] - top)
                    total = total + gain[kb] * totals[kb, h]
                inverse = 1.0 / jnp.sum(total, axis=0, keepdims=True)
                for kb in range(low, qb + 1):
                    scales[b, kb, h] = gain[kb] * inverse
            yield
        low0 = lowest(t * blocks)
        end0 = (t + 1) * blocks
        if mixed is not None:
            for kb in range(mixed, low0):
                for h in range(heads):
                    mix(kb, h, c_s[h, kb * QB : (kb + 1) * QB, :])
        for kb in range(low0, end0):
            if kb == (low0 + end0) // 2:
                yield
            for h in range(heads):
                r = slice(kb * QB, (kb + 1) * QB)
                part = None if kb >= t * blocks else c_s[h, r, :].reshape(QB // 8, 8, QB)
                for b in range(blocks):
                    if (b, kb, h) in scales:
                        low = lowest(t * blocks + b)
                        e = e_s[b, kb - low, h].reshape(QB // 8, 8, QB) * scales[b, kb, h][None]
                        part = e if part is None else part + e
                part = part.reshape(QB, QB)
                c_s[h, r, :] = part
                if mixed is not None and kb >= mixed:
                    mix(kb, h, part)

    bound = (rows - MIN_LEN * (slots - half), rows)
    floor = (0, MIN_LEN * half // QB)
    ready = (-(-bound[0] // tile) - 1, tiles - 1)

    def finish(p):
        low, high = floor[p] * QB, (ready[p] + 1) * tile
        if p == 0:
            yield
            yield
        attended = jnp.dot(
            members(low, high - low), mx_s[low:high, :], preferred_element_type=F32
        )
        upper = attended.astype(BF16)
        lower = attended - upper.astype(F32)
        both = jnp.concatenate([upper.astype(F32), lower], axis=0).astype(BF16)
        reach = list(range(1, n_mp))
        reach.sort(key=lambda d: -min(d, n_mp - d))
        reach.append(0)
        for group in (reach[: n_mp // 2], reach[n_mp // 2 :]):
            for d in group:
                m = lax.rem(rank + d, n_mp)
                cols = pl.ds(pl.multiple_of(m * share, share), share)
                out = jnp.dot(both, wo_s[:, cols], preferred_element_type=F32)
                out = out[:slots] + out[slots:]
                hp_s[p, d] = out[p * half : (p + 1) * half]
            if p == 1:
                for d in group:
                    if d > 0:
                        rs_copy(p, d).start()
            yield

    def signal_all():
        barrier = pltpu.get_barrier_semaphore()
        for d in range(1, n_mp):
            peer = (dp, lax.rem(rank + d, n_mp))
            pl.semaphore_signal(barrier, inc=1, device_id=peer, device_id_type=MESH)
        for d in range(1, n_dp):
            peer = (lax.rem(dp + d, n_dp), rank)
            pl.semaphore_signal(barrier, inc=1, device_id=peer, device_id_type=MESH)

    def rs_copy(p, d):
        peer = lax.rem(rank + d, n_mp)
        return pltpu.make_async_remote_copy(
            src_ref=hp_s.at[p, d], dst_ref=rs_s.at[p, d - 1],
            send_sem=rs_send.at[p, d - 1], recv_sem=rs_recv.at[p, d - 1],
            device_id=(dp, peer), device_id_type=MESH,
        )

    wide = 2 if n_dp % 4 == 0 else 1
    tall = n_dp // (2 * wide)

    def ag_peer(d):
        k = n_dp - 1 - (d - 1)
        c, x, y = k % 2, k // 2 % wide, k // (2 * wide)
        chip = dp // 2
        across = lax.rem(lax.rem(chip, wide) + x, wide)
        down = lax.rem(chip // wide + y, tall)
        return (down * wide + across) * 2 + lax.rem(lax.rem(dp, 2) + c, 2)

    def ag_copy(p, d):
        return pltpu.make_async_remote_copy(
            src_ref=ag_s.at[p, dp], dst_ref=ag_s.at[p, dp],
            send_sem=ag_send.at[p, d - 1], recv_sem=ag_recv.at[p, d - 1],
            device_id=(ag_peer(d), rank), device_id_type=MESH,
        )

    def g_copy(p, d):
        ref = (ga_s, gb_s)[p]
        return pltpu.make_async_remote_copy(
            src_ref=ref.at[rank], dst_ref=ref.at[rank],
            send_sem=g_send.at[p, d - 1], recv_sem=g_recv.at[p, d - 1],
            device_id=(dp, lax.rem(rank + d, n_mp)), device_id_type=MESH,
        )

    def pool(p):
        with jax.named_scope(f"rs{p}"):
            for d in range(1, n_mp):
                rs_copy(p, d).wait_recv()
        slot = lax.broadcasted_iota(jnp.int32, (half, share), 0)
        count = jnp.ones((half, share), F32)
        for j in range(half):
            count = jnp.where(slot == j, ln_ref[p * half + j].astype(F32), count)
        pooled = ts_s[p * half : (p + 1) * half, :] + hp_s[p, 0]
        for d in range(1, n_mp):
            pooled = pooled + rs_s[p, d - 1]
        ag_s[p, dp] = pooled / count
        for d in range(1, n_dp):
            ag_copy(p, d).start()

    def split(a):
        upper = a.astype(BF16)
        return upper, (a - upper.astype(F32)).astype(BF16)

    def product(a, b, axes):
        (ah, al), (bh, bl) = a, b
        where = ((axes[:1], axes[1:]), ((), ()))
        def one(u, w):
            return lax.dot_general(u, w, where, preferred_element_type=F32)
        if al is None:
            return one(ah, bh) + one(ah, bl)
        return one(ah, bh) + (one(ah, bl) + one(al, bh))

    def gathered(p):
        with jax.named_scope(f"ag{p}"):
            for d in range(1, n_dp):
                ag_copy(p, d).wait_recv()
        return split(jnp.concatenate([ag_s[p, d] for d in range(n_dp)], axis=0))

    def folded(a):
        f = max(1, 128 // a.shape[1])
        tall = a.shape[0] // f
        return jnp.concatenate([a[k * tall : (k + 1) * tall] for k in range(f)], axis=1)

    def unfolded(ref, columns):
        total = ref[0]
        for m in range(1, n_mp):
            total = total + ref[m]
        f = total.shape[1] // columns
        return jnp.concatenate(
            [total[:, k * columns : (k + 1) * columns] for k in range(f)], axis=0
        )

    def tail():
        nseq = 2 * near
        pool(0)
        pool(1)
        place = lax.broadcasted_iota(jnp.int32, (nseq, nseq), 1)
        spot = place % near
        origin = (spot // half) * slots + (place // near) * half + spot % half
        order = jnp.where(
            lax.broadcasted_iota(jnp.int32, (nseq, nseq), 0) == origin, 1.0, 0.0
        ).astype(BF16)
        facts = jnp.concatenate(
            [ref[...].astype(F32).reshape(1, nseq) for ref in (ep_ref, cl_ref, fl_ref)]
            + [jnp.zeros((5, nseq), F32)], axis=0,
        ).astype(BF16)
        facts = jnp.dot(facts, order, preferred_element_type=F32)
        episode, label, query = facts[0:1], facts[1:2], facts[2:3]
        label = episode * float(WAYS) + label
        class_row = lax.broadcasted_iota(jnp.int32, (classes, nseq), 0).astype(F32)
        select = jnp.where((class_row == label) & (query == 0.0), 1.0, 0.0)
        a = lax.broadcasted_iota(jnp.int32, (slots, nseq), 0)
        a = (a // half) * near + dp * half + a % half
        mine = a == lax.broadcasted_iota(jnp.int32, (slots, nseq), 1)
        own_query = jnp.sum(jnp.where(mine, query, 0.0), axis=-1, keepdims=True)
        own_episode = jnp.sum(jnp.where(mine, episode, 0.0), axis=-1, keepdims=True)
        eye = lax.broadcasted_iota(jnp.int32, (nseq, nseq), 0) == lax.broadcasted_iota(
            jnp.int32, (nseq, nseq), 1
        )
        eye_c = lax.broadcasted_iota(jnp.int32, (classes, classes), 0) == lax.broadcasted_iota(
            jnp.int32, (classes, classes), 1
        )
        x0 = gathered(0)
        ga_s[rank] = folded(product(x0, x0, (1, 1)))
        for d in range(1, n_mp):
            g_copy(0, d).start()
        x1 = gathered(1)
        gb_s[rank] = folded(
            jnp.concatenate([product(x1, x0, (1, 1)), product(x1, x1, (1, 1))], axis=1)
        )
        for d in range(1, n_mp):
            g_copy(1, d).start()
        every = tuple(jnp.concatenate([u, w], axis=0) for u, w in zip(x0, x1))
        for p in range(2):
            for d in range(1, n_mp):
                rs_copy(p, d).wait_send()
            for d in range(1, n_dp):
                ag_copy(p, d).wait_send()
        with jax.named_scope("gwait"):
            for p in range(2):
                for d in range(1, n_mp):
                    g_copy(p, d).wait_recv()
        with jax.named_scope("score"):
            score(select, every, mine, eye, eye_c, own_query, own_episode)
        for p in range(2):
            for d in range(1, n_mp):
                g_copy(p, d).wait_send()

    def score(select, every, mine, eye, eye_c, own_query, own_episode):
        nseq = 2 * near
        g00 = unfolded(ga_s, near)
        below = unfolded(gb_s, nseq)
        gram = jnp.concatenate(
            [jnp.concatenate([g00, below[:, :near].T], axis=1), below], axis=0
        )
        diag = jnp.where(eye, gram, 0.0)
        norms = jnp.sum(diag, axis=0, keepdims=True)
        scale_row = lax.rsqrt(norms / width + 1e-06)
        norms = norms * scale_row * scale_row
        scale_col = lax.rsqrt(jnp.sum(diag, axis=1, keepdims=True) / width + 1e-06)
        gram = gram * scale_row * scale_col
        cross_t = product((select.astype(BF16), None), split(gram), (1, 0))
        norm_col = jnp.maximum(jnp.sum(cross_t * select, axis=1, keepdims=True), 0.0)
        proto_col = lax.rsqrt(norm_col / width + 1e-06)
        pr_ref[...] = product(split(select * scale_row), every, (1, 0)) * proto_col
        cross = product((mine.astype(F32).astype(BF16), None), split(cross_t), (1, 1))
        norm_row = jnp.sum(jnp.where(eye_c, norm_col, 0.0), axis=0, keepdims=True)
        proto_row = lax.rsqrt(norm_row / width + 1e-06)
        own_norm = jnp.sum(jnp.where(mine, norms, 0.0), axis=-1, keepdims=True)
        distance = own_norm - 2.0 * (cross * proto_row) + norm_row * proto_row * proto_row
        picked = jnp.zeros((slots, WAYS), F32)
        for e in range(classes // WAYS):
            picked = jnp.where(own_episode == float(e), distance[:, e * WAYS : (e + 1) * WAYS], picked)
        logits = -picked / math.sqrt(width)
        shifted = logits - jnp.max(logits, axis=-1, keepdims=True)
        logp = shifted - jnp.log(jnp.sum(jnp.exp(shifted), axis=-1, keepdims=True))
        lp_ref[...] = jnp.where(own_query == 1.0, logp, 0.0)

    for step in range(tiles + 1):
        @pl.when(i == step)
        def _(step=step):
            if step == 0:
                few[0].start()
                for c in range(chunks):
                    head_copy(c).start()
                for copy in w_copies(0):
                    copy.start()
                for copy in few[1:]:
                    copy.start()
                signal_all()
            if 0 < step < tiles - 1:
                x_copy(step + 1).start()
            if step == 2:
                wo_copy.start()
            if step < tiles:
                with jax.named_scope("xwait"):
                    if step == 0:
                        few[0].wait()
                        head_copy(0).wait()
                        if chunks > 1:
                            for copy in w_copies(1):
                                copy.start()
                    else:
                        x_copy(step).wait()
            if step == ready[0] + 2:
                wo_copy.wait()
            with jax.named_scope(f"step{step}"):
                work = []
                if step < tiles:
                    work.append(project(step))
                if step == ready[0] + 2:
                    work.append(finish(0))
                if step > 0:
                    mixed = [floor[p] for p in range(2) if ready[p] == step - 1]
                    work.append(attend(step - 1, mixed[0] if mixed else None))
                while work:
                    work = [w for w in work if next(w, True) is None]
            if step == ready[0] + 2:
                with jax.named_scope("barrier"):
                    pl.semaphore_wait(pltpu.get_barrier_semaphore(), n_mp + n_dp - 2)
                for d in range(1, n_mp):
                    rs_copy(0, d).start()
            if step == tiles:
                with jax.named_scope("finish"):
                    for _ in finish(1):
                        pass
                with jax.named_scope("tail"):
                    tail()


def copy_kernel(a_ref, b_ref, x_ref, y_ref):
    x_ref[...] = a_ref[...]
    y_ref[...] = b_ref[...]


def per_device(
    n_dp, n_mp, tokens, norm_gain, w_query, w_key, w_value, w_out,
    seq_starts, seq_lengths, episode_ids, class_ids, query_flags,
):
    rows, width = tokens.shape
    slots = seq_starts.shape[0]
    hd = HEAD_DIM
    heads = w_query.shape[1] // hd
    assert w_key.shape[1] == hd
    share = width // n_mp
    tile = pick(rows, (256, 128))
    chunk = pick(width, (2048, 512, 256, 128))
    piece = pick(width, (1024, 512, 256, 128))
    frequency = ROPE_BASE ** (-np.arange(hd // 2, dtype=np.float64) * 2.0 / hd)
    angles = np.arange(rows, dtype=np.float64)[:, None] * frequency[None, :]
    trig = jnp.asarray(np.concatenate([np.cos(angles), np.sin(angles)], axis=1), F32)
    vmem = pl.BlockSpec(memory_space=pltpu.VMEM)
    hbm = pl.BlockSpec(memory_space=pl.ANY)
    nseq = episode_ids.shape[0]
    classes = max(1, nseq // (2 * WAYS)) * WAYS
    half = slots // 2
    near = n_dp * half
    fold_a = max(1, 128 // near)
    fold_b = max(1, 128 // nseq)
    span = -(-(MAX_LEN - 1) // QB) + 1
    dma = pltpu.SemaphoreType.DMA
    dims = (rows, tile, width, slots, heads, chunk, piece, share, n_mp, n_dp, classes)
    outs = pl.pallas_call(
        functools.partial(fused_kernel, dims),
        grid=(rows // tile + 1,),
        out_shape=(
            jax.ShapeDtypeStruct((slots, WAYS), F32),
            jax.ShapeDtypeStruct((classes, share), F32),
        ),
        in_specs=[hbm] * 12,
        out_specs=(
            pl.BlockSpec((slots, WAYS), lambda i: (0, 0)),
            pl.BlockSpec((classes, share), lambda i: (0, 0)),
        ),
        scratch_shapes=[
            pltpu.VMEM((rows, width), BF16),
            pltpu.VMEM((tile, width), BF16),
            pltpu.VMEM((width, (heads + 2) * hd), BF16),
            pltpu.VMEM(w_out.shape, BF16),
            pltpu.VMEM((rows, hd), F32),
            pltpu.VMEM((2, tile // QB, hd, heads * QB), BF16),
            pltpu.VMEM((rows, hd), BF16),
            pltpu.VMEM((rows, hd), BF16),
            pltpu.VMEM((tile // QB, span, heads, QB, QB), F32),
            pltpu.VMEM((heads, rows, QB), F32),
            pltpu.VMEM((tile, (heads + 2) * hd), F32),
            pltpu.VMEM((rows, heads * hd), BF16),
            pltpu.VMEM((slots, share), F32),
            pltpu.VMEM((2, n_mp, half, share), F32),
            pltpu.VMEM((2, n_mp - 1, half, share), F32),
            pltpu.VMEM((2, n_dp, half, share), F32),
            pltpu.VMEM((n_mp, near // fold_a, near * fold_a), F32),
            pltpu.VMEM((n_mp, near // fold_b, nseq * fold_b), F32),
            pltpu.SMEM((slots,), jnp.int32),
            pltpu.SMEM((slots,), jnp.int32),
            pltpu.VMEM((width,), BF16),
            pltpu.VMEM((nseq,), jnp.int32),
            pltpu.VMEM((nseq,), jnp.int32),
            pltpu.VMEM((nseq,), jnp.int32),
            dma((6,)),
            dma((rows // tile,)),
            dma((width // chunk,)),
            dma((width // chunk, 3)),
            dma,
            dma,
            dma((2, n_mp - 1)), dma((2, n_mp - 1)),
            dma((2, n_dp - 1)), dma((2, n_dp - 1)),
            dma((2, n_mp - 1)), dma((2, n_mp - 1)),
        ],
        compiler_params=pltpu.CompilerParams(
            dimension_semantics=("arbitrary",), vmem_limit_bytes=60 * 1024 * 1024,
            collective_id=0, has_side_effects=True,
        ),
    )(
        seq_starts, seq_lengths, norm_gain,
        episode_ids, class_ids, query_flags,
        tokens, w_query, w_key, w_value, w_out, trig,
    )
    return pl.pallas_call(
        copy_kernel,
        out_shape=tuple(jax.ShapeDtypeStruct(a.shape, a.dtype) for a in outs),
        in_specs=[vmem, vmem],
        out_specs=(vmem, vmem),
    )(*outs)


def solution(mesh):
    placed = (
        P("dp", None), P(), P(None, "mp"), P(None, "mp"), P(None, "mp"), P("mp", None),
        P("dp"), P("dp"), P(), P(), P(),
    )
    return jax.shard_map(
        functools.partial(per_device, mesh.shape["dp"], mesh.shape["mp"]),
        mesh=mesh,
        in_specs=placed,
        out_specs=(P("dp", None), P(None, "mp")),
        check_vma=False,
    )
```

```python
import functools
import math

import numpy as np
import jax
import jax.numpy as jnp
from jax import lax
from jax.experimental import pallas as pl
from jax.experimental.pallas import tpu as pltpu
from jax.sharding import PartitionSpec as P

HEAD_DIM = 128
WAYS = 32
ROPE_BASE = 500000.0
NEG_FILL = -1e30
MAX_LEN = 640
MIN_LEN = 128
QB = 128
MESH = pl.DeviceIdType.MESH
F32 = jnp.float32
BF16 = jnp.bfloat16
HIGHEST = lax.Precision.HIGHEST


def pick(total, options):
    for candidate in options:
        if total % candidate == 0:
            return candidate
    return total


def fused_kernel(
    dims, st_hbm, ln_hbm, gain_hbm, ep_hbm, cl_hbm, fl_hbm,
    x_hbm, wq_hbm, wk_hbm, wv_hbm, wo_hbm, trig_hbm,
    lp_ref, pr_ref, x_s, xg_s, w_s, wo_s, trig_s, qt_s, k_s, v_s, e_s, c_s, p_s, sq_s, mx_s, ts_s,
    hp_s, rs_s, ag_s, ga_s, gb_s, st_ref, ln_ref, gain_ref, ep_ref, cl_ref, fl_ref,
    few_sem, x_sem, head_sem, w_sem, wo_sem, trig_sem,
    rs_send, rs_recv, ag_send, ag_recv, g_send, g_recv,
):
    rows, tile, width, slots, heads, chunk, piece, share, n_mp, n_dp, classes = dims
    hd = HEAD_DIM
    i = pl.program_id(0)
    tiles = rows // tile
    q_cols = heads * hd
    chunks = width // chunk
    blocks = tile // QB
    far = sorted(range(1, n_mp), key=lambda d: -min(d, n_mp - d))
    slack = rows - MIN_LEN * slots

    def lowest(qb):
        first = qb * QB
        start = max(0, first - MAX_LEN + 1, MIN_LEN * ((first - slack) // MIN_LEN))
        return start // QB

    few = [
        pltpu.make_async_copy(src, dst, few_sem.at[k])
        for k, (src, dst) in enumerate((
            (gain_hbm, gain_ref), (st_hbm, st_ref), (ln_hbm, ln_ref),
            (ep_hbm, ep_ref), (cl_hbm, cl_ref), (fl_hbm, fl_ref),
        ))
    ]

    def head_copy(c):
        at = (pl.ds(0, tile), pl.ds(pl.multiple_of(c * chunk, chunk), chunk))
        return pltpu.make_async_copy(x_hbm.at[at], x_s.at[at], head_sem.at[c])

    half = slots // 2
    near = n_dp * half
    dp = lax.axis_index("dp")
    rank = lax.axis_index("mp")
    wo_copy = pltpu.make_async_copy(wo_hbm, wo_s, wo_sem)

    def trig_copy(k):
        r = pl.ds(0, tile) if k == 0 else pl.ds(tile, rows - tile)
        return pltpu.make_async_copy(trig_hbm.at[r, :], trig_s.at[r, :], trig_sem.at[k])

    def x_copy(t):
        r = pl.ds(t * tile, tile)
        return pltpu.make_async_copy(x_hbm.at[r, :], x_s.at[r, :], x_sem.at[t])

    def w_copies(c):
        r = pl.ds(pl.multiple_of(c * chunk, chunk), chunk)
        return (
            pltpu.make_async_copy(wq_hbm.at[r, :], w_s.at[r, pl.ds(0, q_cols)], w_sem.at[c, 0]),
            pltpu.make_async_copy(wk_hbm.at[r, :], w_s.at[r, pl.ds(q_cols, hd)], w_sem.at[c, 1]),
            pltpu.make_async_copy(wv_hbm.at[r, :], w_s.at[r, pl.ds(q_cols + hd, hd)], w_sem.at[c, 2]),
        )

    def members(first, count):
        slot = lax.broadcasted_iota(jnp.int32, (slots, count), 0)
        token = lax.broadcasted_iota(jnp.int32, (slots, count), 1) + first
        lo = jnp.zeros((slots, count), jnp.int32)
        hi = jnp.zeros((slots, count), jnp.int32)
        for j in range(slots):
            lo = jnp.where(slot == j, st_ref[j], lo)
            hi = jnp.where(slot == j, st_ref[j] + ln_ref[j], hi)
        return jnp.where((token >= lo) & (token < hi), 1.0, 0.0).astype(BF16)

    def project(t):
        r0 = t * tile
        span = chunk if t == 0 else piece
        count = width // span
        sums = [jnp.zeros((QB, 256), F32) for _ in range(blocks)]

        def scale(c):
            for b in range(blocks):
                r = slice(r0 + b * QB, r0 + (b + 1) * QB)
                for v in range(c * span, (c + 1) * span, 1024):
                    pair = []
                    for u in range(v, v + 1024, 256):
                        x = x_s[r, u : u + 256]
                        xg_s[b * QB : (b + 1) * QB, u : u + 256] = x * gain_ref[u : u + 256][None, :]
                        pair.append(x * x)
                    sums[b] = sums[b] + ((pair[0] + pair[1]) + (pair[2] + pair[3])).astype(F32)

        if t == 0:
            def chunk_step(c, carry):
                off = pl.multiple_of(c * chunk, chunk)
                head_copy(c).wait()
                gain = gain_ref[pl.ds(off, chunk)]
                for b in range(blocks):
                    r = slice(b * QB, (b + 1) * QB)
                    total = sq_s[b]
                    for v in range(0, chunk, 1024):
                        pair = []
                        for u in range(v, v + 1024, 256):
                            cols = pl.ds(off + u, 256)
                            x = x_s[r, cols]
                            xg_s[r, cols] = x * gain[u : u + 256][None, :]
                            pair.append(x * x)
                        total = total + ((pair[0] + pair[1]) + (pair[2] + pair[3])).astype(F32)
                    sq_s[b] = total
                for copy in w_copies(c):
                    copy.wait()

                @pl.when(c + 3 < chunks)
                def _():
                    for copy in w_copies(c + 3):
                        copy.start()

                @pl.when(c + 2 == chunks)
                def _():
                    x_copy(1).start()
                    trig_copy(1).start()

                s = pl.ds(off, chunk)
                p_s[...] += jnp.dot(xg_s[:, s], w_s[s, :], preferred_element_type=F32)
                return carry

            with jax.named_scope("first"):
                lax.fori_loop(0, chunks, chunk_step, 0)
            sums = [sq_s[b] for b in range(blocks)]
        else:
            scale(0)
        for c in range(count if t > 0 else 0):
            s = slice(c * span, (c + 1) * span)
            part = jnp.dot(xg_s[:, s], w_s[s, :], preferred_element_type=F32)
            p_s[...] = part if c == 0 else p_s[...] + part
            if c + 1 < count:
                scale(c + 1)
            for _ in range(4 // count):
                yield
        if t == 0:
            with jax.named_scope("trig"):
                trig_copy(0).wait()
                for copy in few[1:]:
                    copy.wait()
        stats = [jnp.sum(a, axis=-1, keepdims=True) for a in sums]
        rstd = lax.rsqrt(jnp.concatenate(stats, axis=0) / width + 1e-05)
        cols = pl.ds(pl.multiple_of(rank * share, share), share)
        ts = jnp.dot(members(r0, tile), x_s[r0 : r0 + tile, cols], preferred_element_type=F32)
        if t == 0:
            ts_s[...] = ts
        else:
            ts_s[...] += ts
        trig = trig_s[r0 : r0 + tile, :]
        turned = pltpu.roll(trig, hd // 2, 1)
        front = lax.broadcasted_iota(jnp.int32, (tile, hd), 1) < hd // 2
        cos = jnp.where(front, trig, turned)
        sin = jnp.where(front, -turned, trig)

        def rope(y):
            return y * cos + pltpu.roll(y, hd // 2, 1) * sin

        q_rstd = rstd * (math.log2(math.e) / math.sqrt(hd))
        for h in range(heads):
            q = rope(p_s[:, h * hd : (h + 1) * hd] * q_rstd)
            for b in range(blocks):
                qt_s[t % 2, b, :, h * QB : (h + 1) * QB] = q[b * QB : (b + 1) * QB].T.astype(BF16)
        k_s[r0 : r0 + tile, :] = rope(p_s[:, q_cols : q_cols + hd] * rstd).astype(BF16)
        v_s[r0 : r0 + tile, :] = (p_s[:, q_cols + hd :] * rstd).astype(BF16)

    def mix(kb, h, part):
        r = slice(kb * QB, (kb + 1) * QB)
        mass = jnp.sum(part, axis=-1, keepdims=True)
        mx_s[r, h * hd : (h + 1) * hd] = (mass * v_s[r, :].astype(F32)).astype(BF16)

    def attend(t, mixed):
        scales = {}
        for b in range(blocks):
            qb = t * blocks + b
            first = qb * QB
            token = lax.broadcasted_iota(jnp.int32, (1, QB), 1) + first
            start = token
            for j in range(slots):
                s0 = st_ref[j]
                start = jnp.where((token >= s0) & (token < s0 + ln_ref[j]), s0, start)
            low = lowest(qb)
            peaks = {}
            totals = {}
            for kb in range(low, qb + 1):
                s_all = jnp.dot(
                    k_s[kb * QB : (kb + 1) * QB, :], qt_s[t % 2, b], preferred_element_type=F32
                )
                row = lax.broadcasted_iota(jnp.int32, (QB, QB), 0) + kb * QB
                ok = row >= start
                if kb == qb:
                    ok = ok & (row <= token)
                for h in range(heads):
                    s = jnp.where(ok, s_all[:, h * QB : (h + 1) * QB], NEG_FILL)
                    s = s.reshape(QB // 8, 8, QB)
                    peak = jnp.max(s, axis=0)
                    e = jnp.exp2(s - peak[None])
                    e_s[b, kb - low, h] = e.reshape(QB, QB)
                    peaks[kb, h] = peak
                    totals[kb, h] = jnp.sum(e, axis=0)
            for h in range(heads):
                top = peaks[low, h]
                for kb in range(low + 1, qb + 1):
                    top = jnp.maximum(top, peaks[kb, h])
                top = jnp.max(top, axis=0, keepdims=True)
                total = jnp.zeros((8, QB), F32)
                gain = {}
                for kb in range(low, qb + 1):
                    gain[kb] = jnp.exp2(peaks[kb, h] - top)
                    total = total + gain[kb] * totals[kb, h]
                inverse = 1.0 / jnp.sum(total, axis=0, keepdims=True)
                for kb in range(low, qb + 1):
                    scales[b, kb, h] = gain[kb] * inverse
            yield
        low0 = lowest(t * blocks)
        end0 = (t + 1) * blocks
        if mixed is not None:
            for kb in range(mixed, low0):
                for h in range(heads):
                    mix(kb, h, c_s[h, kb * QB : (kb + 1) * QB, :])
        for kb in range(low0, end0):
            if kb == (low0 + end0) // 2:
                yield
            for h in range(heads):
                r = slice(kb * QB, (kb + 1) * QB)
                part = None if kb >= t * blocks else c_s[h, r, :].reshape(QB // 8, 8, QB)
                for b in range(blocks):
                    if (b, kb, h) in scales:
                        low = lowest(t * blocks + b)
                        e = e_s[b, kb - low, h].reshape(QB // 8, 8, QB) * scales[b, kb, h][None]
                        part = e if part is None else part + e
                part = part.reshape(QB, QB)
                c_s[h, r, :] = part
                if mixed is not None and kb >= mixed:
                    mix(kb, h, part)

    bound = (rows - MIN_LEN * (slots - half), rows)
    floor = (0, MIN_LEN * half // QB)
    ready = (-(-bound[0] // tile) - 1, tiles - 1)

    def finish(p):
        low, high = floor[p] * QB, (ready[p] + 1) * tile
        if p == 0:
            yield
            yield
        attended = jnp.dot(
            members(low, high - low), mx_s[low:high, :], preferred_element_type=F32
        )
        upper = attended.astype(BF16)
        lower = attended - upper.astype(F32)
        both = jnp.concatenate([upper.astype(F32), lower], axis=0).astype(BF16)
        reach = far + [0]
        for group in (reach[: n_mp // 2], reach[n_mp // 2 :]):
            for d in group:
                m = lax.rem(rank + d, n_mp)
                cols = pl.ds(pl.multiple_of(m * share, share), share)
                out = jnp.dot(both, wo_s[:, cols], preferred_element_type=F32)
                out = out[:slots] + out[slots:]
                hp_s[p, d] = out[p * half : (p + 1) * half]
            if p == 1:
                for d in group:
                    if d > 0:
                        rs_copy(p, d).start()
            yield

    def signal_all():
        barrier = pltpu.get_barrier_semaphore()
        for d in range(1, n_mp):
            peer = (dp, lax.rem(rank + d, n_mp))
            pl.semaphore_signal(barrier, inc=1, device_id=peer, device_id_type=MESH)
        for d in range(1, n_dp):
            peer = (lax.rem(dp + d, n_dp), rank)
            pl.semaphore_signal(barrier, inc=1, device_id=peer, device_id_type=MESH)

    def rs_copy(p, d):
        peer = lax.rem(rank + d, n_mp)
        return pltpu.make_async_remote_copy(
            src_ref=hp_s.at[p, d], dst_ref=rs_s.at[p, d - 1],
            send_sem=rs_send.at[p, d - 1], recv_sem=rs_recv.at[p, d - 1],
            device_id=(dp, peer), device_id_type=MESH,
        )

    wide = 2 if n_dp % 4 == 0 else 1
    tall = n_dp // (2 * wide)

    def ag_peer(d):
        k = n_dp - 1 - (d - 1)
        c, x, y = k % 2, k // 2 % wide, k // (2 * wide)
        chip = dp // 2
        across = lax.rem(lax.rem(chip, wide) + x, wide)
        down = lax.rem(chip // wide + y, tall)
        return (down * wide + across) * 2 + lax.rem(lax.rem(dp, 2) + c, 2)

    def ag_copy(p, d):
        return pltpu.make_async_remote_copy(
            src_ref=ag_s.at[p, dp], dst_ref=ag_s.at[p, dp],
            send_sem=ag_send.at[p, d - 1], recv_sem=ag_recv.at[p, d - 1],
            device_id=(ag_peer(d), rank), device_id_type=MESH,
        )

    def g_copy(p, d):
        ref = (ga_s, gb_s)[p]
        return pltpu.make_async_remote_copy(
            src_ref=ref.at[rank], dst_ref=ref.at[rank],
            send_sem=g_send.at[p, d - 1], recv_sem=g_recv.at[p, d - 1],
            device_id=(dp, lax.rem(rank + d, n_mp)), device_id_type=MESH,
        )

    def pool(p):
        with jax.named_scope(f"rs{p}"):
            for d in range(1, n_mp):
                rs_copy(p, d).wait_recv()
        slot = lax.broadcasted_iota(jnp.int32, (half, share), 0)
        count = jnp.ones((half, share), F32)
        for j in range(half):
            count = jnp.where(slot == j, ln_ref[p * half + j].astype(F32), count)
        pooled = ts_s[p * half : (p + 1) * half, :] + hp_s[p, 0]
        for d in range(1, n_mp):
            pooled = pooled + rs_s[p, d - 1]
        ag_s[p, dp] = pooled / count
        for d in range(1, n_dp):
            ag_copy(p, d).start()

    def split(a):
        upper = a.astype(BF16)
        return upper, (a - upper.astype(F32)).astype(BF16)

    def product(a, b, axes):
        (ah, al), (bh, bl) = a, b
        where = ((axes[:1], axes[1:]), ((), ()))
        def one(u, w):
            return lax.dot_general(u, w, where, preferred_element_type=F32)
        if al is None:
            return one(ah, bh) + one(ah, bl)
        return one(ah, bh) + (one(ah, bl) + one(al, bh))

    def gathered(p):
        with jax.named_scope(f"ag{p}"):
            for d in range(1, n_dp):
                ag_copy(p, d).wait_recv()
        return split(jnp.concatenate([ag_s[p, d] for d in range(n_dp)], axis=0))

    def folded(a):
        f = max(1, 128 // a.shape[1])
        tall = a.shape[0] // f
        return jnp.concatenate([a[k * tall : (k + 1) * tall] for k in range(f)], axis=1)

    def unfolded(ref, columns):
        total = ref[0]
        for m in range(1, n_mp):
            total = total + ref[m]
        f = total.shape[1] // columns
        return jnp.concatenate(
            [total[:, k * columns : (k + 1) * columns] for k in range(f)], axis=0
        )

    def tail():
        nseq = 2 * near
        pool(0)
        pool(1)
        place = lax.broadcasted_iota(jnp.int32, (nseq, nseq), 1)
        spot = place % near
        origin = (spot // half) * slots + (place // near) * half + spot % half
        order = jnp.where(
            lax.broadcasted_iota(jnp.int32, (nseq, nseq), 0) == origin, 1.0, 0.0
        ).astype(BF16)
        facts = jnp.concatenate(
            [ref[...].astype(F32).reshape(1, nseq) for ref in (ep_ref, cl_ref, fl_ref)]
            + [jnp.zeros((5, nseq), F32)], axis=0,
        ).astype(BF16)
        facts = jnp.dot(facts, order, preferred_element_type=F32)
        episode, label, query = facts[0:1], facts[1:2], facts[2:3]
        label = episode * float(WAYS) + label
        class_row = lax.broadcasted_iota(jnp.int32, (classes, nseq), 0).astype(F32)
        select = jnp.where((class_row == label) & (query == 0.0), 1.0, 0.0)
        a = lax.broadcasted_iota(jnp.int32, (slots, nseq), 0)
        a = (a // half) * near + dp * half + a % half
        mine = a == lax.broadcasted_iota(jnp.int32, (slots, nseq), 1)
        own_query = jnp.sum(jnp.where(mine, query, 0.0), axis=-1, keepdims=True)
        own_episode = jnp.sum(jnp.where(mine, episode, 0.0), axis=-1, keepdims=True)
        eye = lax.broadcasted_iota(jnp.int32, (nseq, nseq), 0) == lax.broadcasted_iota(
            jnp.int32, (nseq, nseq), 1
        )
        eye_c = lax.broadcasted_iota(jnp.int32, (classes, classes), 0) == lax.broadcasted_iota(
            jnp.int32, (classes, classes), 1
        )
        x0 = gathered(0)
        ga_s[rank] = folded(product(x0, x0, (1, 1)))
        for d in far:
            g_copy(0, d).start()
        x1 = gathered(1)
        gb_s[rank] = folded(
            jnp.concatenate([product(x1, x0, (1, 1)), product(x1, x1, (1, 1))], axis=1)
        )
        for d in far:
            g_copy(1, d).start()
        every = tuple(jnp.concatenate([u, w], axis=0) for u, w in zip(x0, x1))
        for p in range(2):
            for d in range(1, n_mp):
                rs_copy(p, d).wait_send()
            for d in range(1, n_dp):
                ag_copy(p, d).wait_send()
        with jax.named_scope("gwait"):
            for p in range(2):
                for d in range(1, n_mp):
                    g_copy(p, d).wait_recv()
        with jax.named_scope("score"):
            score(select, every, mine, eye, eye_c, own_query, own_episode)
        for p in range(2):
            for d in range(1, n_mp):
                g_copy(p, d).wait_send()

    def score(select, every, mine, eye, eye_c, own_query, own_episode):
        nseq = 2 * near
        g00 = unfolded(ga_s, near)
        below = unfolded(gb_s, nseq)
        gram = jnp.concatenate(
            [jnp.concatenate([g00, below[:, :near].T], axis=1), below], axis=0
        )
        diag = jnp.where(eye, gram, 0.0)
        norms = jnp.sum(diag, axis=0, keepdims=True)
        scale_row = lax.rsqrt(norms / width + 1e-06)
        norms = norms * scale_row * scale_row
        scale_col = lax.rsqrt(jnp.sum(diag, axis=1, keepdims=True) / width + 1e-06)
        gram = gram * scale_row * scale_col
        cross_t = product((select.astype(BF16), None), split(gram), (1, 0))
        norm_col = jnp.maximum(jnp.sum(cross_t * select, axis=1, keepdims=True), 0.0)
        proto_col = lax.rsqrt(norm_col / width + 1e-06)
        pr_ref[...] = product(split(select * scale_row), every, (1, 0)) * proto_col
        cross = product((mine.astype(F32).astype(BF16), None), split(cross_t), (1, 1))
        norm_row = jnp.sum(jnp.where(eye_c, norm_col, 0.0), axis=0, keepdims=True)
        proto_row = lax.rsqrt(norm_row / width + 1e-06)
        own_norm = jnp.sum(jnp.where(mine, norms, 0.0), axis=-1, keepdims=True)
        distance = own_norm - 2.0 * (cross * proto_row) + norm_row * proto_row * proto_row
        picked = jnp.zeros((slots, WAYS), F32)
        for e in range(classes // WAYS):
            picked = jnp.where(own_episode == float(e), distance[:, e * WAYS : (e + 1) * WAYS], picked)
        logits = -picked / math.sqrt(width)
        shifted = logits - jnp.max(logits, axis=-1, keepdims=True)
        logp = shifted - jnp.log(jnp.sum(jnp.exp(shifted), axis=-1, keepdims=True))
        lp_ref[...] = jnp.where(own_query == 1.0, logp, 0.0)

    for step in range(tiles + 1):
        @pl.when(i == step)
        def _(step=step):
            if step == 0:
                few[0].start()
                for c in range(chunks):
                    head_copy(c).start()
                for c in range(min(3, chunks)):
                    for copy in w_copies(c):
                        copy.start()
                trig_copy(0).start()
                p_s[...] = jnp.zeros_like(p_s)
                sq_s[...] = jnp.zeros_like(sq_s)
                for copy in few[1:]:
                    copy.start()
                signal_all()
            if 0 < step < tiles - 1:
                x_copy(step + 1).start()
            if step == 2:
                wo_copy.start()
            if step < tiles:
                with jax.named_scope("xwait"):
                    if step == 0:
                        few[0].wait()
                    else:
                        x_copy(step).wait()
                    if step == 1:
                        trig_copy(1).wait()
            if step == ready[0] + 2:
                wo_copy.wait()
            with jax.named_scope(f"step{step}"):
                work = []
                if step < tiles:
                    work.append(project(step))
                if step == ready[0] + 2:
                    work.append(finish(0))
                if step > 0:
                    mixed = [floor[p] for p in range(2) if ready[p] == step - 1]
                    work.append(attend(step - 1, mixed[0] if mixed else None))
                while work:
                    work = [w for w in work if next(w, True) is None]
            if step == ready[0] + 2:
                with jax.named_scope("barrier"):
                    pl.semaphore_wait(pltpu.get_barrier_semaphore(), n_mp + n_dp - 2)
                for d in range(1, n_mp):
                    rs_copy(0, d).start()
            if step == tiles:
                with jax.named_scope("finish"):
                    for _ in finish(1):
                        pass
                with jax.named_scope("tail"):
                    tail()


def copy_kernel(a_ref, b_ref, x_ref, y_ref):
    x_ref[...] = a_ref[...]
    y_ref[...] = b_ref[...]


def per_device(
    n_dp, n_mp, tokens, norm_gain, w_query, w_key, w_value, w_out,
    seq_starts, seq_lengths, episode_ids, class_ids, query_flags,
):
    rows, width = tokens.shape
    slots = seq_starts.shape[0]
    hd = HEAD_DIM
    heads = w_query.shape[1] // hd
    assert w_key.shape[1] == hd
    share = width // n_mp
    tile = pick(rows, (256, 128))
    chunk = pick(width, (1024, 512, 256, 128))
    piece = pick(width, (1024, 512, 256, 128))
    frequency = ROPE_BASE ** (-np.arange(hd // 2, dtype=np.float64) * 2.0 / hd)
    angles = np.arange(rows, dtype=np.float64)[:, None] * frequency[None, :]
    trig = jnp.asarray(np.concatenate([np.cos(angles), np.sin(angles)], axis=1), F32)
    vmem = pl.BlockSpec(memory_space=pltpu.VMEM)
    hbm = pl.BlockSpec(memory_space=pl.ANY)
    nseq = episode_ids.shape[0]
    classes = max(1, nseq // (2 * WAYS)) * WAYS
    half = slots // 2
    near = n_dp * half
    fold_a = max(1, 128 // near)
    fold_b = max(1, 128 // nseq)
    span = -(-(MAX_LEN - 1) // QB) + 1
    dma = pltpu.SemaphoreType.DMA
    dims = (rows, tile, width, slots, heads, chunk, piece, share, n_mp, n_dp, classes)
    outs = pl.pallas_call(
        functools.partial(fused_kernel, dims),
        grid=(rows // tile + 1,),
        out_shape=(
            jax.ShapeDtypeStruct((slots, WAYS), F32),
            jax.ShapeDtypeStruct((classes, share), F32),
        ),
        in_specs=[hbm] * 12,
        out_specs=(
            pl.BlockSpec((slots, WAYS), lambda i: (0, 0)),
            pl.BlockSpec((classes, share), lambda i: (0, 0)),
        ),
        scratch_shapes=[
            pltpu.VMEM((rows, width), BF16),
            pltpu.VMEM((tile, width), BF16),
            pltpu.VMEM((width, (heads + 2) * hd), BF16),
            pltpu.VMEM(w_out.shape, BF16),
            pltpu.VMEM((rows, hd), F32),
            pltpu.VMEM((2, tile // QB, hd, heads * QB), BF16),
            pltpu.VMEM((rows, hd), BF16),
            pltpu.VMEM((rows, hd), BF16),
            pltpu.VMEM((tile // QB, span, heads, QB, QB), F32),
            pltpu.VMEM((heads, rows, QB), F32),
            pltpu.VMEM((tile, (heads + 2) * hd), F32),
            pltpu.VMEM((tile // QB, QB, 256), F32),
            pltpu.VMEM((rows, heads * hd), BF16),
            pltpu.VMEM((slots, share), F32),
            pltpu.VMEM((2, n_mp, half, share), F32),
            pltpu.VMEM((2, n_mp - 1, half, share), F32),
            pltpu.VMEM((2, n_dp, half, share), F32),
            pltpu.VMEM((n_mp, near // fold_a, near * fold_a), F32),
            pltpu.VMEM((n_mp, near // fold_b, nseq * fold_b), F32),
            pltpu.SMEM((slots,), jnp.int32),
            pltpu.SMEM((slots,), jnp.int32),
            pltpu.VMEM((width,), BF16),
            pltpu.VMEM((nseq,), jnp.int32),
            pltpu.VMEM((nseq,), jnp.int32),
            pltpu.VMEM((nseq,), jnp.int32),
            dma((6,)),
            dma((rows // tile,)),
            dma((width // chunk,)),
            dma((width // chunk, 3)),
            dma,
            dma((2,)),
            dma((2, n_mp - 1)), dma((2, n_mp - 1)),
            dma((2, n_dp - 1)), dma((2, n_dp - 1)),
            dma((2, n_mp - 1)), dma((2, n_mp - 1)),
        ],
        compiler_params=pltpu.CompilerParams(
            dimension_semantics=("arbitrary",), vmem_limit_bytes=60 * 1024 * 1024,
            collective_id=0, has_side_effects=True,
        ),
    )(
        seq_starts, seq_lengths, norm_gain,
        episode_ids, class_ids, query_flags,
        tokens, w_query, w_key, w_value, w_out, trig,
    )
    return pl.pallas_call(
        copy_kernel,
        out_shape=tuple(jax.ShapeDtypeStruct(a.shape, a.dtype) for a in outs),
        in_specs=[vmem, vmem],
        out_specs=(vmem, vmem),
    )(*outs)


def solution(mesh):
    placed = (
        P("dp", None), P(), P(None, "mp"), P(None, "mp"), P(None, "mp"), P("mp", None),
        P("dp"), P("dp"), P(), P(), P(),
    )
    return jax.shard_map(
        functools.partial(per_device, mesh.shape["dp"], mesh.shape["mp"]),
        mesh=mesh,
        in_specs=placed,
        out_specs=(P("dp", None), P(None, "mp")),
        check_vma=False,
    )
```
